128 devices in a mesh: stage: 4 (over x), expert: 32 (over z, y, core).
Axes of the slice: x: 4, y: 4, z: 4, core: 2. Of those that a mesh axis runs over, the one named last changes fastest.
Arguments:
- w_gate: bfloat16 [4, 32, 1024, 512], P('stage', 'expert')
- w_up: bfloat16 [4, 32, 1024, 512], P('stage', 'expert')
- w_down: bfloat16 [4, 32, 512, 1024], P('stage', 'expert')
- dense: bfloat16 [4, 1024, 1024], P('stage')
- hot_ids: int32 [2], replicated
- spare_map: int32 [128], P(('stage', 'expert'))
Outputs:
- output 1: bfloat16 [4, 128, 1024, 256], P(None, ('stage', 'expert'))
- output 2: bfloat16 [4, 128, 128, 1024], P(None, ('stage', 'expert'))
- output 3: bfloat16 [4, 1024, 1024], replicated
- output 4: bfloat16 [4, 128, 1024, 256], P(None, ('stage', 'expert'))
- output 5: bfloat16 [4, 128, 128, 1024], P(None, ('stage', 'expert'))
All inputs are finite; a program needn't handle non-finite values.
Results may differ from the reference program's by a relative error of at most 0.001.
Values are sent between devices in bfloat16 or wider.
A program may use at most 1 GiB of HBM per device.

```python
import jax
import jax.numpy as jnp

LAYERS = 4
EXPERTS = 32
D_MODEL = 1024
FF_WIDTH = 512
DENSE_WIDTH = 1024
PIECES = 4
STAGES = 4
GROUPS = 32
DEVICES = 128
HOT_UNITS = 2

PIECE_WIDTH = FF_WIDTH // PIECES
UNIT_COUNT = EXPERTS * PIECES
PER_DEVICE = UNIT_COUNT // DEVICES


def draw_placement(base_key):
    key_list = jax.random.split(base_key, 6)
    first_dev = jax.random.randint(key_list[0], (), 0, DEVICES, dtype=jnp.int32)
    shift_stage = jax.random.randint(key_list[1], (), 1, STAGES, dtype=jnp.int32)
    shift_group = jax.random.randint(key_list[2], (), 1, GROUPS, dtype=jnp.int32)
    second_stage = (first_dev // GROUPS + shift_stage) % STAGES
    second_group = (first_dev % GROUPS + shift_group) % GROUPS
    second_dev = second_stage * GROUPS + second_group
    offsets = jax.random.randint(key_list[3], (HOT_UNITS,), 0, PER_DEVICE, dtype=jnp.int32)
    hot_ids = jnp.stack([first_dev, second_dev]) * PER_DEVICE + offsets
    base_map = jax.random.randint(key_list[4], (DEVICES,), -1, HOT_UNITS, dtype=jnp.int32)
    slot_order = jax.random.permutation(key_list[5], DEVICES)
    forced = jnp.concatenate([jnp.arange(HOT_UNITS, dtype=jnp.int32), jnp.full((1,), -1, dtype=jnp.int32)])
    spare_map = base_map.at[slot_order[:HOT_UNITS + 1]].set(forced)
    return hot_ids.astype(jnp.int32), spare_map.astype(jnp.int32)


def setup_inputs(seed: int = 0) -> dict:
    key_list = jax.random.split(jax.random.key(seed), 5)
    expert_shape = (LAYERS, EXPERTS, D_MODEL, FF_WIDTH)
    w_gate = jax.random.normal(key_list[0], expert_shape, jnp.float32).astype(jnp.bfloat16)
    w_up = jax.random.normal(key_list[1], expert_shape, jnp.float32).astype(jnp.bfloat16)
    w_down = jax.random.normal(key_list[2], (LAYERS, EXPERTS, FF_WIDTH, D_MODEL), jnp.float32).astype(jnp.bfloat16)
    dense = jax.random.normal(key_list[3], (LAYERS, D_MODEL, DENSE_WIDTH), jnp.float32).astype(jnp.bfloat16)
    hot_ids, spare_map = draw_placement(key_list[4])
    return {'w_gate': w_gate, 'w_up': w_up, 'w_down': w_down, 'dense': dense, 'hot_ids': hot_ids, 'spare_map': spare_map}


def reference(w_gate, w_up, w_down, dense, hot_ids, spare_map):
    gate_parts = w_gate.reshape(LAYERS, EXPERTS, D_MODEL, PIECES, PIECE_WIDTH)
    up_parts = w_up.reshape(LAYERS, EXPERTS, D_MODEL, PIECES, PIECE_WIDTH)
    gate_up = jnp.concatenate([gate_parts, up_parts], axis=-1)
    gate_up = jnp.transpose(gate_up, (0, 1, 3, 2, 4)).reshape(LAYERS, UNIT_COUNT, D_MODEL, 2 * PIECE_WIDTH)
    down_units = w_down.reshape(LAYERS, UNIT_COUNT, PIECE_WIDTH, D_MODEL)
    hot_gate_up = jnp.take(gate_up, hot_ids, axis=1)
    hot_down = jnp.take(down_units, hot_ids, axis=1)
    slot_index = jnp.maximum(spare_map, 0)
    filled = (spare_map >= 0)[None, :, None, None]
    spare_gate_up = jnp.where(filled, jnp.take(hot_gate_up, slot_index, axis=1), jnp.zeros((), gate_up.dtype))
    spare_down = jnp.where(filled, jnp.take(hot_down, slot_index, axis=1), jnp.zeros((), down_units.dtype))
    return gate_up, down_units, dense, spare_gate_up, spare_down
```

```python
import functools

import jax
import jax.numpy as jnp
from jax import lax
from jax.experimental import pallas as pl
from jax.experimental.pallas import tpu as pltpu
from jax.sharding import PartitionSpec as P

MESH = pl.DeviceIdType.MESH
BF16 = jnp.bfloat16
RING = 4
UNIT_CHUNKS = 6
DENSE_CHUNKS = 8


def _exchange(gate, up, down, dense, hot, b13, b2, h13, h2, dn,
              w13, w2, p13, p2, q13, q2, c13, c2, rz13, rz2, s13, s2, ry13, ry2, ss, rs, ls):
    x = lax.axis_index('stage')
    e = lax.axis_index('expert')
    z, y, c = e // 8, (e % 8) // 2, e % 2

    def dev(xx, yy, zz, cc):
        return (lax.rem(xx + RING, RING), lax.rem(zz + RING, RING) * 8 + lax.rem(yy + RING, RING) * 2 + cc)

    def ring(v):
        return lax.rem(v + RING, RING)

    partner = dev(x, y, z, 1 - c)
    counter = [0]
    pending = []

    def slots(n):
        base = counter[0]
        counter[0] += n
        return base

    def remote(src, dst, device, slot=None, recv=None):
        slot = slots(1) if slot is None else slot
        recv = slot if recv is None else recv
        return pltpu.make_async_remote_copy(src_ref=src, dst_ref=dst, send_sem=ss.at[slot], recv_sem=rs.at[recv],
                                            device_id=device, device_id_type=MESH)

    def go(*copies):
        for copy in copies:
            copy.start()
            pending.append(copy)

    stays = (z == y) & (c == y // 2)

    def land(zs):
        return jnp.where(zs == x, x, RING + zs)

    loads = []
    for p in range(4):
        cols = pl.ds(p * 128, 128)
        loads.append(pltpu.make_async_copy(gate.at[:, :, :, cols], w13.at[p, :, :, :, 0:128], ls.at[p]))
        loads.append(pltpu.make_async_copy(up.at[:, :, :, cols], w13.at[p, :, :, :, 128:256], ls.at[4 + p]))
    loads.append(pltpu.make_async_copy(down, w2, ls.at[8]))
    load_dense = pltpu.make_async_copy(dense, dn.at[x], ls.at[9])
    own_piece = 2 * (y % 2) + c
    own_cols = pl.ds(pl.multiple_of(own_piece * 128, 128), 128)
    keep = [
        pltpu.make_async_copy(gate.at[:, :, :, own_cols], b13.at[land(z), :, :, :, 0:128], ls.at[10]),
        pltpu.make_async_copy(up.at[:, :, :, own_cols], b13.at[land(z), :, :, :, 128:256], ls.at[11]),
        pltpu.make_async_copy(down.at[own_piece], b2.at[land(z)], ls.at[12]),
    ]
    for copy in loads:
        copy.start()
    load_dense.start()

    @pl.when(stays)
    def _():
        for copy in keep:
            copy.start()

    bar = pltpu.get_barrier_semaphore()

    def greet(device):
        pl.semaphore_signal(bar, inc=1, device_id=device, device_id_type=MESH)

    for zs in range(RING):
        @pl.when(jnp.logical_not(stays & (z == zs)))
        def _():
            greet(dev(x, z, zs, y // 2))
    for d in (1, 2, 3):
        greet(dev(x + d, y, z, c))
        greet(dev(x, y + d, z, c))
        greet(dev(x, y, z + d, c))
    greet(partner)

    for copy in loads:
        copy.wait()
    hot_c = hot[c]
    hot_n = hot[1 - c]
    p13[...] = w13[hot_n % 4]
    p2[...] = w2[hot_n % 4]
    pl.semaphore_wait(bar, jnp.where(stays, 13, 14))

    yz_send = slots(4 * UNIT_CHUNKS)
    yz_recv = slots(4 * UNIT_CHUNKS)

    def unit_part(big, small, index, q):
        if q < 4:
            return big.at[index, q]
        return small.at[index, pl.ds(2 * (q - 4), 2)]

    def yz(p, q):
        return remote(unit_part(w13, w2, p, q), unit_part(b13, b2, land(z), q),
                      dev(x, 2 * c + p // 2, y, p % 2), yz_send + p * UNIT_CHUNKS + q, yz_recv + z * UNIT_CHUNKS + q)

    def yz_self(p):
        return stays & (own_piece == p)

    def yz_go(q):
        for p in range(4):
            @pl.when(jnp.logical_not(yz_self(p)))
            def _():
                yz(p, q).start()

    def yz_drain():
        for q in range(UNIT_CHUNKS):
            for p in range(4):
                @pl.when(jnp.logical_not(yz_self(p)))
                def _():
                    yz(p, q).wait_send()

    def yz_arrive(zs, q):
        part = unit_part(b13, b2, land(zs), q)

        @pl.when(jnp.logical_not(stays & (zs == z)))
        def _():
            remote(part, part, partner, yz_send, yz_recv + zs * UNIT_CHUNKS + q).wait_recv()

        if q == 0:
            @pl.when(stays & (zs == z))
            def _():
                for copy in keep:
                    copy.wait()

    def x_make(d, q):
        to = ring(x + d)
        return remote(unit_part(b13, b2, RING + to, q), unit_part(b13, b2, x, q), dev(x + d, y, z, c))

    x_copies = {(d, q): x_make(d, q) for d in (1, 2, 3) for q in range(UNIT_CHUNKS)}

    def x_go(q):
        for d in (1, 3, 2):
            yz_arrive(ring(x + d), q)
            go(x_copies[d, q])

    def dn_part(layer, j, core=None):
        return dn.at[layer, c if core is None else core, j]

    half = DENSE_CHUNKS // 2
    d_right = [remote(dn_part(x, j), dn_part(x, j), dev(x + 1, y, z, c)) for j in range(DENSE_CHUNKS)]
    d_left = [remote(dn_part(x, j), dn_part(x, j), dev(x - 1, y, z, c)) for j in range(DENSE_CHUNKS)]
    d_far = [remote(dn_part(ring(x - 1), j), dn_part(ring(x - 1), j), dev(x + 1, y, z, c)) if j < half else
             remote(dn_part(ring(x + 1), j), dn_part(ring(x + 1), j), dev(x - 1, y, z, c)) for j in range(DENSE_CHUNKS)]
    d_pass = {(d, j): remote(dn_part(ring(x + d), j), dn_part(ring(x + d), j), partner)
              for d in (1, 2, 3) for j in range(DENSE_CHUNKS)}

    def dense_start():
        load_dense.wait()
        for i in range(DENSE_CHUNKS):
            go(d_right[i], d_left[(i + half) % DENSE_CHUNKS])

    def dense_near(i):
        j = (i + half) % DENSE_CHUNKS
        d_right[i].wait_recv()
        if i < half:
            go(d_far[i])
        go(d_pass[3, i])
        d_left[j].wait_recv()
        if j >= half:
            go(d_far[j])
        go(d_pass[1, j])

    def dense_far():
        for j in range(DENSE_CHUNKS):
            d_far[j].wait_recv()
            go(d_pass[2, j])

    def dense_end():
        for copy in d_pass.values():
            copy.wait_recv()

    pq = [remote(p13, q13, partner), remote(p2, q2, partner)]
    rsz = {d: [remote(c13.at[:, ring(z + d)], rz13.at[z], dev(x, y, z + d, c)),
               remote(c2.at[:, ring(z + d)], rz2.at[z], dev(x, y, z + d, c))] for d in (1, 2, 3)}
    rsy = {d: [remote(s13.at[ring(y + d)], ry13.at[y], dev(x, y + d, z, c)),
               remote(s2.at[ring(y + d)], ry2.at[y], dev(x, y + d, z, c))] for d in (1, 2, 3)}
    agx = {d: [remote(h.at[c, x, y, z], h.at[c, x, y, z], dev(x + d, y, z, c)) for h in (h13, h2)] for d in (1, 2, 3)}
    ag1 = {d: [remote(h.at[c, 0:2, y, z], h.at[c, 0:2, y, z], dev(x, y, z + d, c)) for h in (h13, h2)]
           + [remote(h.at[c, 2:4, y, z], h.at[c, 2:4, y, z], dev(x, y + d, z, c)) for h in (h13, h2)] for d in (1, 2, 3)}

    def block(h, layer, d):
        if layer < 2:
            return h.at[c, layer, ring(y + d)]
        return h.at[c, layer, :, ring(z + d)]

    def along(layer, d):
        return dev(x, y + d, z, c) if layer < 2 else dev(x, y, z + d, c)

    ag2 = {(d, l): [remote(block(h, l, 0), block(h, l, 0), along(l, d)) for h in (h13, h2)] for d in (1, -1) for l in range(4)}
    ag3 = {l: [remote(block(h, l, -1 if l % 2 == 0 else 1), block(h, l, -1 if l % 2 == 0 else 1),
                      along(l, 1 if l % 2 == 0 else -1)) for h in (h13, h2)] for l in range(4)}
    h_pass = {(d, l): [remote(block(h, l, d), block(h, l, d), partner) for h in (h13, h2)]
              for d in (0, 1, 2, 3) for l in range(4)}

    def recv(copies):
        for copy in copies:
            copy.wait_recv()

    def hot_swap():
        go(*pq)

    def hot_rsz():
        recv(pq)
        own = (hot_c // 4) % 2 == c
        c13[...] = jnp.where(own, w13[hot_c % 4], q13[...])
        c2[...] = jnp.where(own, w2[hot_c % 4], q2[...])
        rz13[z] = c13[:, z]
        rz2[z] = c2[:, z]
        for d in (1, 3, 2):
            go(*rsz[d])

    def hot_rsy():
        for d in (1, 3, 2):
            recv(rsz[d])
        zh = hot_c // 32
        s13[...] = rz13[zh]
        s2[...] = rz2[zh]
        ry13[y] = s13[y]
        ry2[y] = s2[y]
        for d in (1, 3, 2):
            go(*rsy[d])

    def hot_agx():
        for d in (1, 3, 2):
            recv(rsy[d])
        yh = (hot_c // 8) % 4
        h13[c, x, y, z] = ry13[yh]
        h2[c, x, y, z] = ry2[yh]
        for d in (1, 3, 2):
            go(*agx[d])

    def hot_ag1():
        for d in (1, 3, 2):
            recv(agx[d])
        for d in (1, 3, 2):
            go(*ag1[d])

    def hot_ag2():
        for d in (1, 3, 2):
            recv(ag1[d])
        for l in (0, 2):
            go(*ag2[1, l])
            go(*ag2[-1, l + 1])
        for l in (1, 3):
            go(*ag2[1, l])
            go(*ag2[-1, l - 1])
        for l in range(4):
            go(*h_pass[0, l])

    def hot_ag3():
        for l in (0, 2):
            recv(ag2[1, l])
            go(*ag3[l])
            recv(ag2[-1, l + 1])
            go(*ag3[l + 1])
        for l in (0, 2):
            go(*h_pass[3, l])
            go(*h_pass[1, l + 1])
        for l in (1, 3):
            recv(ag2[1, l])
            go(*h_pass[3, l])
            recv(ag2[-1, l - 1])
            go(*h_pass[1, l - 1])

    def hot_end():
        for l in range(4):
            recv(ag3[l])
            go(*h_pass[2, l])
        for copies in h_pass.values():
            recv(copies)

    hot_swap()
    yz_go(0)
    dense_start()
    hot_rsz()
    yz_go(1)
    yz_go(2)
    hot_rsy()
    yz_go(3)
    dense_near(0)
    x_go(0)
    hot_agx()
    yz_go(4)
    yz_go(5)
    dense_near(1)
    dense_near(2)
    x_go(1)
    hot_ag1()
    dense_near(3)
    x_go(2)
    for i in range(4, 8):
        dense_near(i)
    hot_ag2()
    x_go(3)
    hot_ag3()
    x_go(4)
    x_go(5)
    dense_far()
    hot_end()
    dense_end()
    for q in range(UNIT_CHUNKS):
        yz_arrive(x, q)
    for copy in x_copies.values():
        copy.wait_recv()
    yz_drain()
    for copy in pending:
        copy.wait_send()


def _write(spare, b13, b2, h13, h2, dn, o13, o2, odn, osp13, osp2, zero13, zero2, sem):
    copies = [
        pltpu.make_async_copy(dn, odn, sem.at[0]),
        pltpu.make_async_copy(b13.at[0:4], o13, sem.at[1]),
        pltpu.make_async_copy(b2.at[0:4], o2, sem.at[2]),
    ]
    for copy in copies:
        copy.start()
    slot = spare[0]

    @pl.when(slot >= 0)
    def _():
        fill = [pltpu.make_async_copy(h13.at[slot], osp13, sem.at[3]), pltpu.make_async_copy(h2.at[slot], osp2, sem.at[4])]
        for copy in fill:
            copy.start()
        for copy in fill:
            copy.wait()

    @pl.when(slot < 0)
    def _():
        zero13[...] = jnp.zeros_like(zero13)
        zero2[...] = jnp.zeros_like(zero2)
        fill = [pltpu.make_async_copy(zero13, osp13.at[l, m], sem.at[5 + 4 * l + m]) for l in range(4) for m in range(4)]
        fill += [pltpu.make_async_copy(zero2, osp2.at[l], sem.at[21 + l]) for l in range(4)]
        for copy in fill:
            copy.start()
        for copy in fill:
            copy.wait()

    for copy in copies:
        copy.wait()


def solution(mesh):
    flat_axes = ('stage', 'expert')

    def local_move(w_gate, w_up, w_down, dense, hot_ids, spare_map):
        gate = w_gate.reshape(4, 4, 64, 512)
        up = w_up.reshape(4, 4, 64, 512)
        down = w_down.reshape(4, 4, 4, 8, 1024)
        dense_in = dense.reshape(2, DENSE_CHUNKS, 64, 1024)
        hbm = pl.BlockSpec(memory_space=pltpu.HBM)
        vmem = pl.BlockSpec(memory_space=pltpu.VMEM)
        smem = pl.BlockSpec(memory_space=pltpu.SMEM)
        count = 400
        moved = pl.pallas_call(
            _exchange,
            name='exchange',
            out_shape=(
                pltpu.VMEM((8, 4, 4, 64, 256), BF16),
                pltpu.VMEM((8, 4, 4, 8, 1024), BF16),
                pltpu.VMEM((2, 4, 4, 4, 64, 256), BF16),
                pltpu.VMEM((2, 4, 4, 4, 8, 1024), BF16),
                pltpu.VMEM((4, 2, DENSE_CHUNKS, 64, 1024), BF16),
            ),
            in_specs=[hbm] * 4 + [smem],
            out_specs=[vmem] * 5,
            scratch_shapes=[
                pltpu.VMEM((4, 4, 4, 64, 256), BF16), pltpu.VMEM((4, 4, 4, 8, 1024), BF16),
                pltpu.VMEM((4, 4, 64, 256), BF16), pltpu.VMEM((4, 4, 8, 1024), BF16),
                pltpu.VMEM((4, 4, 64, 256), BF16), pltpu.VMEM((4, 4, 8, 1024), BF16),
                pltpu.VMEM((4, 4, 64, 256), BF16), pltpu.VMEM((4, 4, 8, 1024), BF16),
                pltpu.VMEM((4, 4, 64, 256), BF16), pltpu.VMEM((4, 4, 8, 1024), BF16),
                pltpu.VMEM((4, 64, 256), BF16), pltpu.VMEM((4, 8, 1024), BF16),
                pltpu.VMEM((4, 64, 256), BF16), pltpu.VMEM((4, 8, 1024), BF16),
                pltpu.SemaphoreType.DMA((count,)), pltpu.SemaphoreType.DMA((count,)), pltpu.SemaphoreType.DMA((13,)),
            ],
            compiler_params=pltpu.CompilerParams(collective_id=0, has_side_effects=True, vmem_limit_bytes=16 * 2**20),
        )(*[pltpu.with_memory_space_constraint(part, pltpu.HBM) for part in (gate, up, down, dense_in)], hot_ids)
        moved = [pltpu.with_memory_space_constraint(part, pltpu.VMEM) for part in moved]
        o13, o2, odn, osp13, osp2 = pl.pallas_call(
            _write,
            name='write',
            out_shape=(
                jax.ShapeDtypeStruct((4, 4, 4, 64, 256), BF16),
                jax.ShapeDtypeStruct((4, 4, 4, 8, 1024), BF16),
                jax.ShapeDtypeStruct((4, 2, DENSE_CHUNKS, 64, 1024), BF16),
                jax.ShapeDtypeStruct((4, 4, 4, 64, 256), BF16),
                jax.ShapeDtypeStruct((4, 4, 4, 8, 1024), BF16),
            ),
            in_specs=[smem] + [vmem] * 5,
            out_specs=[hbm] * 5,
            scratch_shapes=[pltpu.VMEM((4, 64, 256), BF16), pltpu.VMEM((4, 4, 8, 1024), BF16), pltpu.SemaphoreType.DMA((25,))],
            compiler_params=pltpu.CompilerParams(vmem_limit_bytes=4 * 2**20),
        )(spare_map, *moved)
        return (o13.reshape(4, 1, 1024, 256), o2.reshape(4, 1, 128, 1024), odn.reshape(4, 1024, 1024),
                osp13.reshape(4, 1, 1024, 256), osp2.reshape(4, 1, 128, 1024))

    expert_spec = P('stage', 'expert', None, None)
    unit_spec = P(None, flat_axes, None, None)
    return jax.shard_map(
        local_move,
        mesh=mesh,
        in_specs=(expert_spec, expert_spec, expert_spec, P('stage', None, None), P(None), P(flat_axes)),
        out_specs=(unit_spec, unit_spec, P(None, None, None), unit_spec, unit_spec),
        check_vma=False,
    )
```

```python
import jax
import jax.numpy as jnp
from jax import lax
from jax.experimental import pallas as pl
from jax.experimental.pallas import tpu as pltpu
from jax.sharding import PartitionSpec as P

MESH = pl.DeviceIdType.MESH
BF16 = jnp.bfloat16
RING = 4
UNIT_CHUNKS = 8
NEAR_CHUNKS = 8
NEAR_ROWS = 48
SIDE_ROWS = 16


def _exchange(gate, up, down, dense, hot, b, h, dn, u, give, take_in, cand, rza, ryb, sa, sb, rya, rzb, send, recv, local):
    x = lax.axis_index('stage')
    e = lax.axis_index('expert')
    z, y, c = e // 8, (e % 8) // 2, e % 2

    def ring(v):
        return lax.rem(v + RING, RING)

    def dev(xx, yy, zz, cc):
        return (ring(xx), ring(zz) * 8 + ring(yy) * 2 + cc)

    partner = dev(x, y, z, 1 - c)
    S_YZ, S_X, S_DENSE, S_HOT, S_MID, S_LOW = range(6)
    R_YZ = 0
    R_NEAR = R_YZ + RING * UNIT_CHUNKS
    R_FAR = R_NEAR + 2 * NEAR_CHUNKS
    R_AG2 = R_FAR + NEAR_CHUNKS
    R_AG3 = R_AG2 + 8
    R_X, R_CROSS, R_SIDE, R_DPASS, R_HPASS, R_SWAP, R_RS1, R_RS2, R_AGX, R_AG1 = range(R_AG3 + 4, R_AG3 + 14)

    def remote(src, dst, device, s, r):
        return pltpu.make_async_remote_copy(src_ref=src, dst_ref=dst, send_sem=send.at[s], recv_sem=recv.at[r],
                                            device_id=device, device_id_type=MESH)

    def same(ref, device, s, r):
        return remote(ref, ref, device, s, r)

    def settle(sem, like):
        pltpu.make_async_copy(like, like, sem).wait()

    stays = (z == y) & (c == y // 2)
    own_piece = 2 * (y % 2) + c

    def land(zs):
        return jnp.where(zs == x, x, RING + zs)

    loads = []
    for p in range(4):
        cols = pl.ds(p * 128, 128)
        loads.append(pltpu.make_async_copy(gate.at[:, :, :, cols], u.at[p, :, :, 0:64, 0:128], local.at[0]))
        loads.append(pltpu.make_async_copy(up.at[:, :, :, cols], u.at[p, :, :, 0:64, 128:256], local.at[0]))
        for a in range(4):
            loads.append(pltpu.make_async_copy(down.at[p, :, :, :, pl.ds(256 * a, 256)],
                                               u.at[p, :, :, pl.ds(64 + 8 * a, 8), :], local.at[0]))
    own_cols = pl.ds(pl.multiple_of(own_piece * 128, 128), 128)
    keep = [
        pltpu.make_async_copy(gate.at[:, :, :, own_cols], b.at[land(z), :, :, 0:64, 0:128], local.at[1]),
        pltpu.make_async_copy(up.at[:, :, :, own_cols], b.at[land(z), :, :, 0:64, 128:256], local.at[1]),
    ] + [
        pltpu.make_async_copy(down.at[own_piece, :, :, :, pl.ds(256 * a, 256)],
                              b.at[land(z), :, :, pl.ds(64 + 8 * a, 8), :], local.at[1]) for a in range(4)
    ]
    load_dense = pltpu.make_async_copy(dense, dn.at[x], local.at[2])
    for copy in loads:
        copy.start()
    load_dense.start()

    @pl.when(stays)
    def _():
        for copy in keep:
            copy.start()

    bar = pltpu.get_barrier_semaphore()

    def greet(device):
        pl.semaphore_signal(bar, inc=1, device_id=device, device_id_type=MESH)

    for zs in range(RING):
        @pl.when(jnp.logical_not(stays & (z == zs)))
        def _():
            greet(dev(x, z, zs, y // 2))
    for d in (1, 2, 3):
        greet(dev(x + d, y, z, c))
        greet(dev(x, y + d, z, c))
        greet(dev(x, y, z + d, c))
    greet(partner)

    settle(local.at[0], u)
    hot_c = hot[c]
    give[...] = u[hot[1 - c] % 4]
    pl.semaphore_wait(bar, jnp.where(stays, 13, 14))

    def part(ref, index, q):
        return ref.at[index, q // 2, pl.ds(2 * (q % 2), 2)]

    def yz_self(p):
        return stays & (own_piece == p)

    def yz_go(*chunks):
        for q in chunks:
            for p in range(4):
                @pl.when(jnp.logical_not(yz_self(p)))
                def _():
                    remote(part(u, p, q), part(b, land(z), q), dev(x, 2 * c + p // 2, y, p % 2),
                           S_YZ, R_YZ + z * UNIT_CHUNKS + q).start()

    def yz_arrive(zs, q):
        @pl.when(jnp.logical_not(stays & (zs == z)))
        def _():
            settle(recv.at[R_YZ + zs * UNIT_CHUNKS + q], part(b, land(zs), q))

        if q == 0:
            @pl.when(stays & (zs == z))
            def _():
                settle(local.at[1], b.at[0])

    def x_go(*chunks):
        for q in chunks:
            for d in (1, 3, 2):
                to = ring(x + d)
                yz_arrive(to, q)
                remote(part(b, RING + to, q), part(b, x, q), dev(x + d, y, z, c), S_X, R_X).start()

    def near(layer, j):
        return dn.at[ring(layer), c, pl.ds(NEAR_ROWS * j, NEAR_ROWS)]

    side_y = NEAR_ROWS * NEAR_CHUNKS + SIDE_ROWS * y
    side_z = NEAR_ROWS * NEAR_CHUNKS + SIDE_ROWS * (RING + z)

    def side(layer, start):
        return dn.at[ring(layer), c, pl.ds(pl.multiple_of(start, SIDE_ROWS), SIDE_ROWS)]

    half = NEAR_CHUNKS // 2

    def dense_wait():
        load_dense.wait()

    def dense_cross():
        for d in (1, 3, 2):
            for start in (side_y, side_z):
                same(side(x, start), dev(x + d, y, z, c), S_DENSE, R_CROSS).start()

    def dense_own(*chunks):
        for i in chunks:
            j = (i + half) % NEAR_CHUNKS
            same(near(x, i), dev(x + 1, y, z, c), S_DENSE, R_NEAR + i).start()
            same(near(x, j), dev(x - 1, y, z, c), S_DENSE, R_NEAR + NEAR_CHUNKS + j).start()

    def dense_side():
        settle(recv.at[R_CROSS], b.at[0, 0])
        for d in (1, 3, 2):
            for l in (1, 3, 2):
                same(side(x + l, side_y), dev(x, y + d, z, c), S_DENSE, R_SIDE).start()
                same(side(x + l, side_z), dev(x, y, z + d, c), S_DENSE, R_SIDE).start()

    def dense_side_end():
        settle(recv.at[R_SIDE], b.at[0, 0:3])
        for l in (1, 3, 2):
            same(dn.at[ring(x + l), c, pl.ds(NEAR_ROWS * NEAR_CHUNKS, 2 * RING * SIDE_ROWS)], partner, S_DENSE, R_DPASS).start()

    def dense_near(*chunks):
        for i in chunks:
            j = (i + half) % NEAR_CHUNKS
            settle(recv.at[R_NEAR + i], near(x - 1, i))
            if i < half:
                same(near(x - 1, i), dev(x + 1, y, z, c), S_DENSE, R_FAR + i).start()
            same(near(x - 1, i), partner, S_DENSE, R_DPASS).start()
            settle(recv.at[R_NEAR + NEAR_CHUNKS + j], near(x + 1, j))
            if j >= half:
                same(near(x + 1, j), dev(x - 1, y, z, c), S_DENSE, R_FAR + j).start()
            same(near(x + 1, j), partner, S_DENSE, R_DPASS).start()

    def dense_far():
        for j in range(NEAR_CHUNKS):
            settle(recv.at[R_FAR + j], near(x + 2, j))
            same(near(x + 2, j), partner, S_DENSE, R_DPASS).start()

    y_hot, z_hot = (hot_c // 8) % 4, hot_c // 32

    def hot_swap():
        remote(give, take_in, partner, S_HOT, R_SWAP).start()

    def hot_rs1():
        settle(recv.at[R_SWAP], take_in)
        cand[...] = jnp.where((hot_c // 4) % 2 == c, u[hot_c % 4], take_in[...])
        rza[z] = cand[:, z, 0:48]
        ryb[y] = cand[y, :, 48:96]
        for d in (1, 3, 2):
            remote(cand.at[:, ring(z + d), 0:48], rza.at[z], dev(x, y, z + d, c), S_MID, R_RS1).start()
            remote(cand.at[ring(y + d), :, 48:96], ryb.at[y], dev(x, y + d, z, c), S_MID, R_RS1).start()

    def hot_rs2():
        settle(recv.at[R_RS1], b.at[0, 0:3])
        sa[...] = rza[z_hot]
        sb[...] = ryb[y_hot]
        rya[y] = sa[y]
        rzb[z] = sb[z]
        for d in (1, 3, 2):
            remote(sa.at[ring(y + d)], rya.at[y], dev(x, y + d, z, c), S_LOW, R_RS2).start()
            remote(sb.at[ring(z + d)], rzb.at[z], dev(x, y, z + d, c), S_LOW, R_RS2).start()

    def hot_agx():
        settle(recv.at[R_RS2], b.at[0, 0, 0:3])
        h[c, x, y, z, 0:48] = rya[y_hot]
        h[c, x, y, z, 48:96] = rzb[z_hot]
        for d in (1, 3, 2):
            same(h.at[c, x, y, z], dev(x + d, y, z, c), S_LOW, R_AGX).start()

    def hot_ag1():
        settle(recv.at[R_AGX], b.at[0, 0, 0:3])
        for d in (1, 3, 2):
            same(h.at[c, 0:2, y, z], dev(x, y, z + d, c), S_MID, R_AG1).start()
            same(h.at[c, 2:4, y, z], dev(x, y + d, z, c), S_MID, R_AG1).start()

    def block(layer, d):
        if layer < 2:
            return h.at[c, layer, ring(y + d)]
        return h.at[c, layer, :, ring(z + d)]

    def along(layer, d):
        return dev(x, y + d, z, c) if layer < 2 else dev(x, y, z + d, c)

    def hot_ag2():
        settle(recv.at[R_AG1], b.at[0, 0:3])
        for lift in (0, 1):
            for l in (0, 2):
                same(block(l + lift, 0), along(l, 1), S_HOT, R_AG2 + l + lift).start()
                same(block(l + 1 - lift, 0), along(l, -1), S_HOT, R_AG2 + 4 + l + 1 - lift).start()
        for l in range(4):
            same(block(l, 0), partner, S_HOT, R_HPASS).start()

    def hot_ag3():
        for lift in (0, 1):
            for l in (0, 2):
                settle(recv.at[R_AG2 + l + lift], block(l + lift, -1))
                if lift == 0:
                    same(block(l, -1), along(l, 1), S_HOT, R_AG3 + l).start()
                same(block(l + lift, -1), partner, S_HOT, R_HPASS).start()
                settle(recv.at[R_AG2 + 4 + l + 1 - lift], block(l + 1 - lift, 1))
                if lift == 0:
                    same(block(l + 1, 1), along(l, -1), S_HOT, R_AG3 + l + 1).start()
                same(block(l + 1 - lift, 1), partner, S_HOT, R_HPASS).start()

    def hot_end():
        for l in range(4):
            settle(recv.at[R_AG3 + l], block(l, 2))
            same(block(l, 2), partner, S_HOT, R_HPASS).start()

    dense_wait()
    hot_swap()
    yz_go(0)
    dense_cross()
    dense_own(0, 1, 2, 3, 4, 5, 6, 7)
    hot_rs1()
    yz_go(1)
    hot_rs2()
    yz_go(2)
    hot_agx()
    yz_go(3)
    dense_near(0, 1, 2, 3, 4, 5, 6, 7)
    x_go(0, 1)
    hot_ag1()
    yz_go(4, 5)
    x_go(2)
    dense_side()
    x_go(3)
    hot_ag2()
    yz_go(6, 7)
    x_go(4, 5)
    dense_side_end()
    hot_ag3()
    x_go(6, 7)
    dense_far()
    hot_end()
    for q in range(UNIT_CHUNKS):
        yz_arrive(x, q)
    settle(recv.at[R_X], b.at[0:3])
    settle(recv.at[R_DPASS], b.at[0:4])
    settle(recv.at[R_HPASS], b.at[0:4])

    @pl.when(stays)
    def _():
        settle(send.at[S_YZ], b.at[0:3])

    @pl.when(jnp.logical_not(stays))
    def _():
        settle(send.at[S_YZ], b.at[0:4])

    settle(send.at[S_X], b.at[0:3])
    settle(send.at[S_DENSE], b)
    settle(send.at[S_HOT], b)
    settle(send.at[S_MID], b.at[0:2, 0:3])
    settle(send.at[S_LOW], b.at[0:2, 0, 0:3])


def _write(spare, b, h, dn, o13, o2, odn, osp13, osp2, zero13, zero2, sem):
    copies = [pltpu.make_async_copy(dn, odn, sem.at[0])]
    copies.append(pltpu.make_async_copy(b.at[0:4, :, :, 0:64], o13, sem.at[1]))
    for a in range(4):
        copies.append(pltpu.make_async_copy(b.at[0:4, :, :, pl.ds(64 + 8 * a, 8)], o2.at[:, :, :, :, pl.ds(256 * a, 256)], sem.at[2 + a]))
    for copy in copies:
        copy.start()
    slot = spare[0]

    @pl.when(slot >= 0)
    def _():
        fill = [pltpu.make_async_copy(h.at[slot, :, :, :, 0:64], osp13, sem.at[6])]
        for a in range(4):
            fill.append(pltpu.make_async_copy(h.at[slot, :, :, :, pl.ds(64 + 8 * a, 8)], osp2.at[:, :, :, :, pl.ds(256 * a, 256)], sem.at[7 + a]))
        for copy in fill:
            copy.start()
        for copy in fill:
            copy.wait()

    @pl.when(slot < 0)
    def _():
        zero13[...] = jnp.zeros_like(zero13)
        zero2[...] = jnp.zeros_like(zero2)
        fill = [pltpu.make_async_copy(zero13, osp13.at[l], sem.at[6 + l]) for l in range(4)]
        fill += [pltpu.make_async_copy(zero2, osp2.at[l], sem.at[10 + l]) for l in range(4)]
        for copy in fill:
            copy.start()
        for copy in fill:
            copy.wait()

    for copy in copies:
        copy.wait()


def solution(mesh):
    flat_axes = ('stage', 'expert')

    def local_move(w_gate, w_up, w_down, dense, hot_ids, spare_map):
        sources = (w_gate.reshape(4, 4, 64, 512), w_up.reshape(4, 4, 64, 512), w_down.reshape(4, 4, 4, 8, 1024),
                   dense.reshape(2, 512, 1024))
        hbm = pl.BlockSpec(memory_space=pltpu.HBM)
        vmem = pl.BlockSpec(memory_space=pltpu.VMEM)
        smem = pl.BlockSpec(memory_space=pltpu.SMEM)
        unit = (4, 4, 96, 256)
        moved = pl.pallas_call(
            _exchange,
            name='exchange',
            out_shape=(pltpu.VMEM((8,) + unit, BF16), pltpu.VMEM((2, 4) + unit, BF16), pltpu.VMEM((4, 2, 512, 1024), BF16)),
            in_specs=[hbm] * 4 + [smem],
            out_specs=[vmem] * 3,
            scratch_shapes=[
                pltpu.VMEM((4,) + unit, BF16), pltpu.VMEM(unit, BF16), pltpu.VMEM(unit, BF16), pltpu.VMEM(unit, BF16),
                pltpu.VMEM((4, 4, 48, 256), BF16), pltpu.VMEM((4, 4, 48, 256), BF16),
                pltpu.VMEM((4, 48, 256), BF16), pltpu.VMEM((4, 48, 256), BF16),
                pltpu.VMEM((4, 48, 256), BF16), pltpu.VMEM((4, 48, 256), BF16),
                pltpu.SemaphoreType.DMA((6,)),
                pltpu.SemaphoreType.DMA((4 * UNIT_CHUNKS + 3 * NEAR_CHUNKS + 22,)),
                pltpu.SemaphoreType.DMA((3,)),
            ],
            compiler_params=pltpu.CompilerParams(collective_id=0, has_side_effects=True, vmem_limit_bytes=16 * 2**20),
        )(*[pltpu.with_memory_space_constraint(part, pltpu.HBM) for part in sources], hot_ids)
        moved = [pltpu.with_memory_space_constraint(part, pltpu.VMEM) for part in moved]
        o13, o2, odn, osp13, osp2 = pl.pallas_call(
            _write,
            name='write',
            out_shape=(
                jax.ShapeDtypeStruct((4, 4, 4, 64, 256), BF16),
                jax.ShapeDtypeStruct((4, 4, 4, 8, 1024), BF16),
                jax.ShapeDtypeStruct((4, 2, 512, 1024), BF16),
                jax.ShapeDtypeStruct((4, 4, 4, 64, 256), BF16),
                jax.ShapeDtypeStruct((4, 4, 4, 8, 1024), BF16),
            ),
            in_specs=[smem] + [vmem] * 3,
            out_specs=[hbm] * 5,
            scratch_shapes=[pltpu.VMEM((4, 4, 64, 256), BF16), pltpu.VMEM((4, 4, 8, 1024), BF16), pltpu.SemaphoreType.DMA((14,))],
            compiler_params=pltpu.CompilerParams(vmem_limit_bytes=4 * 2**20),
        )(spare_map, *moved)
        return (o13.reshape(4, 1, 1024, 256), o2.reshape(4, 1, 128, 1024), odn.reshape(4, 1024, 1024),
                osp13.reshape(4, 1, 1024, 256), osp2.reshape(4, 1, 128, 1024))

    expert_spec = P('stage', 'expert', None, None)
    unit_spec = P(None, flat_axes, None, None)
    return jax.shard_map(
        local_move,
        mesh=mesh,
        in_specs=(expert_spec, expert_spec, expert_spec, P('stage', None, None), P(None), P(flat_axes)),
        out_specs=(unit_spec, unit_spec, P(None, None, None), unit_spec, unit_spec),
        check_vma=False,
    )
```

```python
import jax
import jax.numpy as jnp
from jax import lax
from jax.experimental import pallas as pl
from jax.experimental.pallas import tpu as pltpu
from jax.sharding import PartitionSpec as P

MESH = pl.DeviceIdType.MESH
BF16 = jnp.bfloat16
RING = 4
UNIT_CHUNKS = 8
NEAR_CHUNKS = 8
NEAR_ROWS = 48
SIDE_ROWS = 16


def _exchange(gate, up, down, dense, hot_hbm, b, h, dn, u, give, take_in, cand, rza, ryb, sa, sb, rya, rzb, ids, send, recv, local):
    x = lax.axis_index('stage')
    e = lax.axis_index('expert')
    z, y, c = e // 8, (e % 8) // 2, e % 2

    def ring(v):
        return lax.rem(v + RING, RING)

    def dev(xx, yy, zz, cc):
        return (ring(xx), ring(zz) * 8 + ring(yy) * 2 + cc)

    partner = dev(x, y, z, 1 - c)
    S_YZ, S_X, S_DENSE, S_HOT, S_MID, S_LOW = range(6)
    R_YZ = 0
    R_NEAR = R_YZ + RING * UNIT_CHUNKS
    R_FAR = R_NEAR + 2 * NEAR_CHUNKS
    R_AG2 = R_FAR + NEAR_CHUNKS
    R_AG3 = R_AG2 + 8
    R_SIDE = R_AG3 + 4
    R_X, R_CROSS, R_TURN, R_DPASS, R_HPASS, R_SWAP, R_RS1, R_RS2, R_AGX, R_AG1 = range(R_SIDE + 4, R_SIDE + 14)

    def remote(src, dst, device, s, r):
        return pltpu.make_async_remote_copy(src_ref=src, dst_ref=dst, send_sem=send.at[s], recv_sem=recv.at[r],
                                            device_id=device, device_id_type=MESH)

    def same(ref, device, s, r):
        return remote(ref, ref, device, s, r)

    def settle(sem, like):
        pltpu.make_async_copy(like, like, sem).wait()

    stays = (z == y) & (c == y // 2)
    own_piece = 2 * (y % 2) + c

    def land(zs):
        return jnp.where(zs == x, x, RING + zs)

    loads = []
    for p in range(4):
        cols = pl.ds(p * 128, 128)
        loads.append(pltpu.make_async_copy(gate.at[:, :, :, cols], u.at[p, :, :, 0:64, 0:128], local.at[0]))
        loads.append(pltpu.make_async_copy(up.at[:, :, :, cols], u.at[p, :, :, 0:64, 128:256], local.at[0]))
        for a in range(4):
            loads.append(pltpu.make_async_copy(down.at[p, :, :, :, pl.ds(256 * a, 256)],
                                               u.at[p, :, :, pl.ds(64 + 8 * a, 8), :], local.at[0]))
    own_cols = pl.ds(pl.multiple_of(own_piece * 128, 128), 128)
    keep = [
        pltpu.make_async_copy(gate.at[:, :, :, own_cols], b.at[land(z), :, :, 0:64, 0:128], local.at[1]),
        pltpu.make_async_copy(up.at[:, :, :, own_cols], b.at[land(z), :, :, 0:64, 128:256], local.at[1]),
    ] + [
        pltpu.make_async_copy(down.at[own_piece, :, :, :, pl.ds(256 * a, 256)],
                              b.at[land(z), :, :, pl.ds(64 + 8 * a, 8), :], local.at[1]) for a in range(4)
    ]
    load_dense = pltpu.make_async_copy(dense, dn.at[x], local.at[2])
    load_ids = pltpu.make_async_copy(hot_hbm, ids, local.at[3])
    load_ids.start()
    for copy in loads:
        copy.start()
    load_dense.start()

    @pl.when(stays)
    def _():
        for copy in keep:
            copy.start()

    bar = pltpu.get_barrier_semaphore()

    def greet(device):
        pl.semaphore_signal(bar, inc=1, device_id=device, device_id_type=MESH)

    for zs in range(RING):
        @pl.when(jnp.logical_not(stays & (z == zs)))
        def _():
            greet(dev(x, z, zs, y // 2))
    for d in (1, 2, 3):
        greet(dev(x + d, y, z, c))
        greet(dev(x, y + d, z, c))
        greet(dev(x, y, z + d, c))
    greet(partner)

    settle(local.at[0], u)
    load_ids.wait()
    hot_c = ids[c]
    give[...] = u[ids[1 - c] % 4]
    pl.semaphore_wait(bar, jnp.where(stays, 13, 14))

    def part(ref, index, q):
        return ref.at[index, q // 2, pl.ds(2 * (q % 2), 2)]

    def yz_self(p):
        return stays & (own_piece == p)

    def yz_go(*chunks):
        for q in chunks:
            for p in range(4):
                @pl.when(jnp.logical_not(yz_self(p)))
                def _():
                    remote(part(u, p, q), part(b, land(z), q), dev(x, 2 * c + p // 2, y, p % 2),
                           S_YZ, R_YZ + z * UNIT_CHUNKS + q).start()

    def yz_arrive(zs, q):
        @pl.when(jnp.logical_not(stays & (zs == z)))
        def _():
            settle(recv.at[R_YZ + zs * UNIT_CHUNKS + q], part(b, land(zs), q))

        if q == 0:
            @pl.when(stays & (zs == z))
            def _():
                settle(local.at[1], b.at[0])

    def x_go(*chunks):
        for q in chunks:
            for d in (1, 3, 2):
                to = ring(x + d)
                yz_arrive(to, q)
                remote(part(b, RING + to, q), part(b, x, q), dev(x + d, y, z, c), S_X, R_X).start()

    def near(layer, j):
        return dn.at[ring(layer), c, pl.ds(NEAR_ROWS * j, NEAR_ROWS)]

    def side(layer, axis, at, lanes=pl.ds(0, 1024)):
        start = NEAR_ROWS * NEAR_CHUNKS + SIDE_ROWS * (RING * axis + ring(at))
        return dn.at[ring(layer), c, pl.ds(pl.multiple_of(start, 8), SIDE_ROWS), lanes]

    def beside(axis, d):
        return dev(x, y, z + d, c) if axis else dev(x, y + d, z, c)

    half = NEAR_CHUNKS // 2

    def dense_wait():
        load_dense.wait()

    def dense_cross():
        for d in (1, 3, 2):
            for axis, at in ((0, y), (1, z)):
                same(side(x, axis, at), dev(x + d, y, z, c), S_DENSE, R_CROSS).start()

    def dense_own(*chunks):
        for i in chunks:
            j = (i + half) % NEAR_CHUNKS
            same(near(x, i), dev(x + 1, y, z, c), S_DENSE, R_NEAR + i).start()
            same(near(x, j), dev(x - 1, y, z, c), S_DENSE, R_NEAR + NEAR_CHUNKS + j).start()

    def dense_side():
        settle(recv.at[R_CROSS], b.at[0, 0])
        for axis, at in ((0, y), (1, z)):
            for d in (1, -1):
                for l in (1, 3, 2):
                    same(side(x + l, axis, at), beside(axis, d), S_DENSE, R_SIDE + 2 * axis + (d + 1) // 2).start()

    def dense_turn():
        for axis, at in ((0, y), (1, z)):
            for d in (1, -1):
                settle(recv.at[R_SIDE + 2 * axis + (d + 1) // 2], b.at[0, 0, 0:2])
                lanes = pl.ds(256 * (1 - d), 512)
                for l in (1, 3, 2):
                    same(side(x + l, axis, at - d, lanes), beside(axis, d), S_DENSE, R_TURN).start()

    def dense_side_end():
        settle(recv.at[R_TURN], b.at[0, 0])
        for l in (1, 3, 2):
            same(dn.at[ring(x + l), c, pl.ds(NEAR_ROWS * NEAR_CHUNKS, 2 * RING * SIDE_ROWS)], partner, S_DENSE, R_DPASS).start()

    def dense_near(*chunks):
        for i in chunks:
            j = (i + half) % NEAR_CHUNKS
            settle(recv.at[R_NEAR + i], near(x - 1, i))
            if i < half:
                same(near(x - 1, i), dev(x + 1, y, z, c), S_DENSE, R_FAR + i).start()
            same(near(x - 1, i), partner, S_DENSE, R_DPASS).start()
            settle(recv.at[R_NEAR + NEAR_CHUNKS + j], near(x + 1, j))
            if j >= half:
                same(near(x + 1, j), dev(x - 1, y, z, c), S_DENSE, R_FAR + j).start()
            same(near(x + 1, j), partner, S_DENSE, R_DPASS).start()

    def dense_far(*chunks):
        for j in chunks:
            settle(recv.at[R_FAR + j], near(x + 2, j))
            same(near(x + 2, j), partner, S_DENSE, R_DPASS).start()

    y_hot, z_hot = (hot_c // 8) % 4, hot_c // 32

    def hot_swap():
        remote(give, take_in, partner, S_HOT, R_SWAP).start()

    def hot_rs1():
        settle(recv.at[R_SWAP], take_in)
        cand[...] = jnp.where((hot_c // 4) % 2 == c, u[hot_c % 4], take_in[...])
        rza[z] = cand[:, z, 0:48]
        ryb[y] = cand[y, :, 48:96]
        for d in (1, 3, 2):
            remote(cand.at[:, ring(z + d), 0:48], rza.at[z], dev(x, y, z + d, c), S_MID, R_RS1).start()
            remote(cand.at[ring(y + d), :, 48:96], ryb.at[y], dev(x, y + d, z, c), S_MID, R_RS1).start()

    def hot_rs2():
        settle(recv.at[R_RS1], b.at[0, 0:3])
        sa[...] = rza[z_hot]
        sb[...] = ryb[y_hot]
        rya[y] = sa[y]
        rzb[z] = sb[z]
        for d in (1, 3, 2):
            remote(sa.at[ring(y + d)], rya.at[y], dev(x, y + d, z, c), S_LOW, R_RS2).start()
            remote(sb.at[ring(z + d)], rzb.at[z], dev(x, y, z + d, c), S_LOW, R_RS2).start()

    def hot_agx():
        settle(recv.at[R_RS2], b.at[0, 0, 0:3])
        h[c, x, y, z, 0:48] = rya[y_hot]
        h[c, x, y, z, 48:96] = rzb[z_hot]
        for d in (1, 3, 2):
            same(h.at[c, x, y, z], dev(x + d, y, z, c), S_LOW, R_AGX).start()

    def hot_ag1():
        settle(recv.at[R_AGX], b.at[0, 0, 0:3])
        for d in (1, 3, 2):
            same(h.at[c, 0:2, y, z], dev(x, y, z + d, c), S_MID, R_AG1).start()
            same(h.at[c, 2:4, y, z], dev(x, y + d, z, c), S_MID, R_AG1).start()

    def block(layer, d):
        if layer < 2:
            return h.at[c, layer, ring(y + d)]
        return h.at[c, layer, :, ring(z + d)]

    def along(layer, d):
        return dev(x, y + d, z, c) if layer < 2 else dev(x, y, z + d, c)

    def hot_ag2():
        settle(recv.at[R_AG1], b.at[0, 0:3])
        for lift in (0, 1):
            for l in (0, 2):
                same(block(l + lift, 0), along(l, 1), S_HOT, R_AG2 + l + lift).start()
                same(block(l + 1 - lift, 0), along(l, -1), S_HOT, R_AG2 + 4 + l + 1 - lift).start()
        for l in range(4):
            same(block(l, 0), partner, S_HOT, R_HPASS).start()

    def hot_ag3(*lifts):
        for lift in lifts:
            for l in (0, 2):
                settle(recv.at[R_AG2 + l + lift], block(l + lift, -1))
                if lift == 0:
                    same(block(l, -1), along(l, 1), S_HOT, R_AG3 + l).start()
                same(block(l + lift, -1), partner, S_HOT, R_HPASS).start()
                settle(recv.at[R_AG2 + 4 + l + 1 - lift], block(l + 1 - lift, 1))
                if lift == 0:
                    same(block(l + 1, 1), along(l, -1), S_HOT, R_AG3 + l + 1).start()
                same(block(l + 1 - lift, 1), partner, S_HOT, R_HPASS).start()

    def hot_end():
        for l in range(4):
            settle(recv.at[R_AG3 + l], block(l, 2))
            same(block(l, 2), partner, S_HOT, R_HPASS).start()

    dense_wait()
    hot_swap()
    yz_go(0)
    dense_cross()
    dense_own(0, 1, 2, 3, 4, 5, 6, 7)
    hot_rs1()
    yz_go(1)
    hot_rs2()
    yz_go(2)
    hot_agx()
    yz_go(3)
    dense_near(0, 1, 2, 3, 4, 5, 6, 7)
    dense_side()
    x_go(0, 1)
    hot_ag1()
    yz_go(4, 5)
    x_go(2, 3)
    dense_turn()
    yz_go(6, 7)
    x_go(4, 5)
    hot_ag2()
    x_go(6, 7)
    hot_ag3(0, 1)
    dense_far(0, 1, 2, 3, 4, 5, 6, 7)
    dense_side_end()
    hot_end()
    for q in range(UNIT_CHUNKS):
        yz_arrive(x, q)
    settle(recv.at[R_X], b.at[0:3])
    settle(recv.at[R_DPASS], b.at[0:4])
    settle(recv.at[R_HPASS], b.at[0:4])

    @pl.when(stays)
    def _():
        settle(send.at[S_YZ], b.at[0:3])

    @pl.when(jnp.logical_not(stays))
    def _():
        settle(send.at[S_YZ], b.at[0:4])

    settle(send.at[S_X], b.at[0:3])
    settle(send.at[S_DENSE], b)
    settle(send.at[S_HOT], b)
    settle(send.at[S_MID], b.at[0:2, 0:3])
    settle(send.at[S_LOW], b.at[0:2, 0, 0:3])


def _write(spare, b, h, dn, o13, o2, odn, osp13, osp2, zero13, zero2, sem):
    copies = [pltpu.make_async_copy(dn, odn, sem.at[0])]
    copies.append(pltpu.make_async_copy(b.at[0:4, :, :, 0:64], o13, sem.at[1]))
    for a in range(4):
        copies.append(pltpu.make_async_copy(b.at[0:4, :, :, pl.ds(64 + 8 * a, 8)], o2.at[:, :, :, :, pl.ds(256 * a, 256)], sem.at[2 + a]))
    for copy in copies:
        copy.start()
    slot = spare[0]

    @pl.when(slot >= 0)
    def _():
        fill = [pltpu.make_async_copy(h.at[slot, :, :, :, 0:64], osp13, sem.at[6])]
        for a in range(4):
            fill.append(pltpu.make_async_copy(h.at[slot, :, :, :, pl.ds(64 + 8 * a, 8)], osp2.at[:, :, :, :, pl.ds(256 * a, 256)], sem.at[7 + a]))
        for copy in fill:
            copy.start()
        for copy in fill:
            copy.wait()

    @pl.when(slot < 0)
    def _():
        zero13[...] = jnp.zeros_like(zero13)
        zero2[...] = jnp.zeros_like(zero2)
        fill = [pltpu.make_async_copy(zero13, osp13.at[l], sem.at[6 + l]) for l in range(4)]
        fill += [pltpu.make_async_copy(zero2, osp2.at[l], sem.at[10 + l]) for l in range(4)]
        for copy in fill:
            copy.start()
        for copy in fill:
            copy.wait()

    for copy in copies:
        copy.wait()


def solution(mesh):
    flat_axes = ('stage', 'expert')

    def local_move(w_gate, w_up, w_down, dense, hot_ids, spare_map):
        sources = (w_gate.reshape(4, 4, 64, 512), w_up.reshape(4, 4, 64, 512), w_down.reshape(4, 4, 4, 8, 1024),
                   dense.reshape(2, 512, 1024))
        hbm = pl.BlockSpec(memory_space=pltpu.HBM)
        vmem = pl.BlockSpec(memory_space=pltpu.VMEM)
        smem = pl.BlockSpec(memory_space=pltpu.SMEM)
        unit = (4, 4, 96, 256)
        moved = pl.pallas_call(
            _exchange,
            name='exchange',
            out_shape=(pltpu.VMEM((8,) + unit, BF16), pltpu.VMEM((2, 4) + unit, BF16), pltpu.VMEM((4, 2, 512, 1024), BF16)),
            in_specs=[hbm] * 5,
            out_specs=[vmem] * 3,
            scratch_shapes=[
                pltpu.VMEM((4,) + unit, BF16), pltpu.VMEM(unit, BF16), pltpu.VMEM(unit, BF16), pltpu.VMEM(unit, BF16),
                pltpu.VMEM((4, 4, 48, 256), BF16), pltpu.VMEM((4, 4, 48, 256), BF16),
                pltpu.VMEM((4, 48, 256), BF16), pltpu.VMEM((4, 48, 256), BF16),
                pltpu.VMEM((4, 48, 256), BF16), pltpu.VMEM((4, 48, 256), BF16),
                pltpu.SMEM((2,), jnp.int32),
                pltpu.SemaphoreType.DMA((6,)),
                pltpu.SemaphoreType.DMA((4 * UNIT_CHUNKS + 3 * NEAR_CHUNKS + 26,)),
                pltpu.SemaphoreType.DMA((4,)),
            ],
            compiler_params=pltpu.CompilerParams(collective_id=0, has_side_effects=True, vmem_limit_bytes=16 * 2**20),
        )(*[pltpu.with_memory_space_constraint(part, pltpu.HBM) for part in (*sources, hot_ids)])
        moved = [pltpu.with_memory_space_constraint(part, pltpu.VMEM) for part in moved]
        o13, o2, odn, osp13, osp2 = pl.pallas_call(
            _write,
            name='write',
            out_shape=(
                jax.ShapeDtypeStruct((4, 4, 4, 64, 256), BF16),
                jax.ShapeDtypeStruct((4, 4, 4, 8, 1024), BF16),
                jax.ShapeDtypeStruct((4, 2, 512, 1024), BF16),
                jax.ShapeDtypeStruct((4, 4, 4, 64, 256), BF16),
                jax.ShapeDtypeStruct((4, 4, 4, 8, 1024), BF16),
            ),
            in_specs=[smem] + [vmem] * 3,
            out_specs=[hbm] * 5,
            scratch_shapes=[pltpu.VMEM((4, 4, 64, 256), BF16), pltpu.VMEM((4, 4, 8, 1024), BF16), pltpu.SemaphoreType.DMA((14,))],
            compiler_params=pltpu.CompilerParams(vmem_limit_bytes=4 * 2**20),
        )(spare_map, *moved)
        return (o13.reshape(4, 1, 1024, 256), o2.reshape(4, 1, 128, 1024), odn.reshape(4, 1024, 1024),
                osp13.reshape(4, 1, 1024, 256), osp2.reshape(4, 1, 128, 1024))

    expert_spec = P('stage', 'expert', None, None)
    unit_spec = P(None, flat_axes, None, None)
    return jax.shard_map(
        local_move,
        mesh=mesh,
        in_specs=(expert_spec, expert_spec, expert_spec, P('stage', None, None), P(None), P(flat_axes)),
        out_specs=(unit_spec, unit_spec, P(None, None, None), unit_spec, unit_spec),
        check_vma=False,
    )
```

```python
import jax
import jax.numpy as jnp
from jax import lax
from jax.experimental import pallas as pl
from jax.experimental.pallas import tpu as pltpu
from jax.sharding import PartitionSpec as P

MESH = pl.DeviceIdType.MESH
BF16 = jnp.bfloat16
RING = 4
UNIT_CHUNKS = 8
NEAR_CHUNKS = 8
NEAR_ROWS = 48
SIDE_ROWS = 16


def _exchange(gate, up, down, dense, hot_hbm, b, h, dn, u, give, take_in, cand, rza, ryb, sa, sb, rya, rzb, ids, send, recv, local):
    x = lax.axis_index('stage')
    e = lax.axis_index('expert')
    z, y, c = e // 8, (e % 8) // 2, e % 2

    def ring(v):
        return lax.rem(v + RING, RING)

    def dev(xx, yy, zz, cc):
        return (ring(xx), ring(zz) * 8 + ring(yy) * 2 + cc)

    partner = dev(x, y, z, 1 - c)
    S_YZ, S_X, S_DENSE, S_HOT, S_MID, S_LOW = range(6)
    R_YZ = 0
    R_NEAR = R_YZ + RING * UNIT_CHUNKS
    R_FAR = R_NEAR + 2 * NEAR_CHUNKS
    R_AG2 = R_FAR + NEAR_CHUNKS
    R_AG3 = R_AG2 + 8
    R_SIDE = R_AG3 + 4
    R_CROSS = R_SIDE + 4
    R_X, R_OVER, R_TURN, R_DPASS, R_HPASS, R_SWAP, R_RS1, R_RS2, R_AGX, R_AG1 = range(R_CROSS + 2, R_CROSS + 12)

    def remote(src, dst, device, s, r):
        return pltpu.make_async_remote_copy(src_ref=src, dst_ref=dst, send_sem=send.at[s], recv_sem=recv.at[r],
                                            device_id=device, device_id_type=MESH)

    def same(ref, device, s, r):
        return remote(ref, ref, device, s, r)

    def settle(sem, like):
        pltpu.make_async_copy(like, like, sem).wait()

    stays = (z == y) & (c == y // 2)
    own_piece = 2 * (y % 2) + c

    def land(zs):
        return jnp.where(zs == x, x, RING + zs)

    loads = []
    for p in range(4):
        cols = pl.ds(p * 128, 128)
        loads.append(pltpu.make_async_copy(gate.at[:, :, :, cols], u.at[p, :, :, 0:64, 0:128], local.at[0]))
        loads.append(pltpu.make_async_copy(up.at[:, :, :, cols], u.at[p, :, :, 0:64, 128:256], local.at[0]))
        for a in range(4):
            loads.append(pltpu.make_async_copy(down.at[p, :, :, :, pl.ds(256 * a, 256)],
                                               u.at[p, :, :, pl.ds(64 + 8 * a, 8), :], local.at[0]))
    own_cols = pl.ds(pl.multiple_of(own_piece * 128, 128), 128)
    keep = [
        pltpu.make_async_copy(gate.at[:, :, :, own_cols], b.at[land(z), :, :, 0:64, 0:128], local.at[1]),
        pltpu.make_async_copy(up.at[:, :, :, own_cols], b.at[land(z), :, :, 0:64, 128:256], local.at[1]),
    ] + [
        pltpu.make_async_copy(down.at[own_piece, :, :, :, pl.ds(256 * a, 256)],
                              b.at[land(z), :, :, pl.ds(64 + 8 * a, 8), :], local.at[1]) for a in range(4)
    ]
    load_dense = pltpu.make_async_copy(dense, dn.at[x], local.at[2])
    load_ids = pltpu.make_async_copy(hot_hbm, ids, local.at[3])
    load_ids.start()
    for copy in loads:
        copy.start()
    load_dense.start()

    @pl.when(stays)
    def _():
        for copy in keep:
            copy.start()

    bar = pltpu.get_barrier_semaphore()

    def greet(device):
        pl.semaphore_signal(bar, inc=1, device_id=device, device_id_type=MESH)

    for zs in range(RING):
        @pl.when(jnp.logical_not(stays & (z == zs)))
        def _():
            greet(dev(x, z, zs, y // 2))
    for d in (1, 2, 3):
        greet(dev(x + d, y, z, c))
        greet(dev(x, y + d, z, c))
        greet(dev(x, y, z + d, c))
    greet(partner)

    settle(local.at[0], u)
    load_ids.wait()
    hot_c = ids[c]
    give[...] = u[ids[1 - c] % 4]
    pl.semaphore_wait(bar, jnp.where(stays, 13, 14))

    def part(ref, index, q):
        return ref.at[index, q // 2, pl.ds(2 * (q % 2), 2)]

    def yz_self(p):
        return stays & (own_piece == p)

    def yz_go(*chunks):
        for q in chunks:
            for p in range(4):
                @pl.when(jnp.logical_not(yz_self(p)))
                def _():
                    remote(part(u, p, q), part(b, land(z), q), dev(x, 2 * c + p // 2, y, p % 2),
                           S_YZ, R_YZ + z * UNIT_CHUNKS + q).start()

    def yz_arrive(zs, q):
        @pl.when(jnp.logical_not(stays & (zs == z)))
        def _():
            settle(recv.at[R_YZ + zs * UNIT_CHUNKS + q], part(b, land(zs), q))

        if q == 0:
            @pl.when(stays & (zs == z))
            def _():
                settle(local.at[1], b.at[0])

    def x_go(*chunks):
        for q in chunks:
            for d in (1, 3, 2):
                to = ring(x + d)
                yz_arrive(to, q)
                remote(part(b, RING + to, q), part(b, x, q), dev(x + d, y, z, c), S_X, R_X).start()

    def near(layer, j):
        return dn.at[ring(layer), c, pl.ds(NEAR_ROWS * j, NEAR_ROWS)]

    def side(layer, axis, at, lanes=pl.ds(0, 1024)):
        start = NEAR_ROWS * NEAR_CHUNKS + SIDE_ROWS * (RING * axis + ring(at))
        return dn.at[ring(layer), c, pl.ds(pl.multiple_of(start, 8), SIDE_ROWS), lanes]

    def beside(axis, d):
        return dev(x, y, z + d, c) if axis else dev(x, y + d, z, c)

    half = NEAR_CHUNKS // 2

    def dense_wait():
        load_dense.wait()

    def dense_cross():
        for d in (1, -1):
            for axis, at in ((0, y), (1, z)):
                same(side(x, axis, at), dev(x + d, y, z, c), S_DENSE, R_CROSS + (d + 1) // 2).start()

    def dense_over():
        for d in (1, -1):
            settle(recv.at[R_CROSS + (d + 1) // 2], dn.at[0, 0, 0:2 * SIDE_ROWS])
            for axis, at in ((0, y), (1, z)):
                same(side(x - d, axis, at, pl.ds(256 * (1 - d), 512)), dev(x + d, y, z, c), S_DENSE, R_OVER).start()

    def dense_own(*chunks):
        for i in chunks:
            j = (i + half) % NEAR_CHUNKS
            same(near(x, i), dev(x + 1, y, z, c), S_DENSE, R_NEAR + i).start()
            same(near(x, j), dev(x - 1, y, z, c), S_DENSE, R_NEAR + NEAR_CHUNKS + j).start()

    def dense_side():
        settle(recv.at[R_OVER], dn.at[0, 0, 0:2 * SIDE_ROWS])
        for axis, at in ((0, y), (1, z)):
            for d in (1, -1):
                for l in (1, 3, 2):
                    same(side(x + l, axis, at), beside(axis, d), S_DENSE, R_SIDE + 2 * axis + (d + 1) // 2).start()

    def dense_turn():
        for axis, at in ((0, y), (1, z)):
            for d in (1, -1):
                settle(recv.at[R_SIDE + 2 * axis + (d + 1) // 2], b.at[0, 0, 0:2])
                lanes = pl.ds(256 * (1 - d), 512)
                for l in (1, 3, 2):
                    same(side(x + l, axis, at - d, lanes), beside(axis, d), S_DENSE, R_TURN).start()

    def dense_side_end():
        settle(recv.at[R_TURN], b.at[0, 0])
        for l in (1, 3, 2):
            same(dn.at[ring(x + l), c, pl.ds(NEAR_ROWS * NEAR_CHUNKS, 2 * RING * SIDE_ROWS)], partner, S_DENSE, R_DPASS).start()

    def dense_near(*chunks):
        for i in chunks:
            j = (i + half) % NEAR_CHUNKS
            settle(recv.at[R_NEAR + i], near(x - 1, i))
            if i < half:
                same(near(x - 1, i), dev(x + 1, y, z, c), S_DENSE, R_FAR + i).start()
            same(near(x - 1, i), partner, S_DENSE, R_DPASS).start()
            settle(recv.at[R_NEAR + NEAR_CHUNKS + j], near(x + 1, j))
            if j >= half:
                same(near(x + 1, j), dev(x - 1, y, z, c), S_DENSE, R_FAR + j).start()
            same(near(x + 1, j), partner, S_DENSE, R_DPASS).start()

    def dense_far(*chunks):
        for j in chunks:
            settle(recv.at[R_FAR + j], near(x + 2, j))
            same(near(x + 2, j), partner, S_DENSE, R_DPASS).start()

    y_hot, z_hot = (hot_c // 8) % 4, hot_c // 32

    def hot_swap():
        remote(give, take_in, partner, S_HOT, R_SWAP).start()

    def hot_rs1():
        settle(recv.at[R_SWAP], take_in)
        cand[...] = jnp.where((hot_c // 4) % 2 == c, u[hot_c % 4], take_in[...])
        rza[z] = cand[:, z, 0:48]
        ryb[y] = cand[y, :, 48:96]
        for d in (1, 3, 2):
            remote(cand.at[:, ring(z + d), 0:48], rza.at[z], dev(x, y, z + d, c), S_MID, R_RS1).start()
            remote(cand.at[ring(y + d), :, 48:96], ryb.at[y], dev(x, y + d, z, c), S_MID, R_RS1).start()

    def hot_rs2():
        settle(recv.at[R_RS1], b.at[0, 0:3])
        sa[...] = rza[z_hot]
        sb[...] = ryb[y_hot]
        rya[y] = sa[y]
        rzb[z] = sb[z]
        for d in (1, 3, 2):
            remote(sa.at[ring(y + d)], rya.at[y], dev(x, y + d, z, c), S_LOW, R_RS2).start()
            remote(sb.at[ring(z + d)], rzb.at[z], dev(x, y, z + d, c), S_LOW, R_RS2).start()

    def hot_agx():
        settle(recv.at[R_RS2], b.at[0, 0, 0:3])
        h[c, x, y, z, 0:48] = rya[y_hot]
        h[c, x, y, z, 48:96] = rzb[z_hot]
        for d in (1, 3, 2):
            same(h.at[c, x, y, z], dev(x + d, y, z, c), S_LOW, R_AGX).start()

    def hot_ag1():
        settle(recv.at[R_AGX], b.at[0, 0, 0:3])
        for d in (1, 3, 2):
            same(h.at[c, 0:2, y, z], dev(x, y, z + d, c), S_MID, R_AG1).start()
            same(h.at[c, 2:4, y, z], dev(x, y + d, z, c), S_MID, R_AG1).start()

    def block(layer, d):
        if layer < 2:
            return h.at[c, layer, ring(y + d)]
        return h.at[c, layer, :, ring(z + d)]

    def along(layer, d):
        return dev(x, y + d, z, c) if layer < 2 else dev(x, y, z + d, c)

    def hot_ag2():
        settle(recv.at[R_AG1], b.at[0, 0:3])
        for lift in (0, 1):
            for l in (0, 2):
                same(block(l + lift, 0), along(l, 1), S_HOT, R_AG2 + l + lift).start()
                same(block(l + 1 - lift, 0), along(l, -1), S_HOT, R_AG2 + 4 + l + 1 - lift).start()
        for l in range(4):
            same(block(l, 0), partner, S_HOT, R_HPASS).start()

    def hot_ag3(*lifts):
        for lift in lifts:
            for l in (0, 2):
                settle(recv.at[R_AG2 + l + lift], block(l + lift, -1))
                if lift == 0:
                    same(block(l, -1), along(l, 1), S_HOT, R_AG3 + l).start()
                same(block(l + lift, -1), partner, S_HOT, R_HPASS).start()
                settle(recv.at[R_AG2 + 4 + l + 1 - lift], block(l + 1 - lift, 1))
                if lift == 0:
                    same(block(l + 1, 1), along(l, -1), S_HOT, R_AG3 + l + 1).start()
                same(block(l + 1 - lift, 1), partner, S_HOT, R_HPASS).start()

    def hot_end():
        for l in range(4):
            settle(recv.at[R_AG3 + l], block(l, 2))
            same(block(l, 2), partner, S_HOT, R_HPASS).start()

    dense_wait()
    hot_swap()
    dense_cross()
    dense_own(0, 1, 2, 3, 4, 5, 6, 7)
    yz_go(0)
    hot_rs1()
    yz_go(1)
    hot_rs2()
    dense_over()
    yz_go(2)
    dense_near(0)
    hot_agx()
    yz_go(3)
    dense_near(1, 2, 3, 4, 5, 6, 7)
    dense_side()
    x_go(0, 1)
    hot_ag1()
    yz_go(4, 5)
    x_go(2, 3)
    dense_turn()
    yz_go(6, 7)
    x_go(4, 5)
    hot_ag2()
    x_go(6)
    dense_far(0, 1, 2, 3, 4, 5, 6, 7)
    x_go(7)
    dense_side_end()
    hot_ag3(0, 1)
    hot_end()
    for q in range(UNIT_CHUNKS):
        yz_arrive(x, q)
    settle(recv.at[R_X], b.at[0:3])
    settle(recv.at[R_DPASS], b.at[0:4])
    settle(recv.at[R_HPASS], b.at[0:4])

    @pl.when(stays)
    def _():
        settle(send.at[S_YZ], b.at[0:3])

    @pl.when(jnp.logical_not(stays))
    def _():
        settle(send.at[S_YZ], b.at[0:4])

    settle(send.at[S_X], b.at[0:3])
    settle(send.at[S_DENSE], b)
    settle(send.at[S_HOT], b)
    settle(send.at[S_MID], b.at[0:2, 0:3])
    settle(send.at[S_LOW], b.at[0:2, 0, 0:3])


def _write(spare, b, h, dn, o13, o2, odn, osp13, osp2, zero13, zero2, sem):
    copies = [pltpu.make_async_copy(dn, odn, sem.at[0])]
    copies.append(pltpu.make_async_copy(b.at[0:4, :, :, 0:64], o13, sem.at[1]))
    for a in range(4):
        copies.append(pltpu.make_async_copy(b.at[0:4, :, :, pl.ds(64 + 8 * a, 8)], o2.at[:, :, :, :, pl.ds(256 * a, 256)], sem.at[2 + a]))
    for copy in copies:
        copy.start()
    slot = spare[0]

    @pl.when(slot >= 0)
    def _():
        fill = [pltpu.make_async_copy(h.at[slot, :, :, :, 0:64], osp13, sem.at[6])]
        for a in range(4):
            fill.append(pltpu.make_async_copy(h.at[slot, :, :, :, pl.ds(64 + 8 * a, 8)], osp2.at[:, :, :, :, pl.ds(256 * a, 256)], sem.at[7 + a]))
        for copy in fill:
            copy.start()
        for copy in fill:
            copy.wait()

    @pl.when(slot < 0)
    def _():
        zero13[...] = jnp.zeros_like(zero13)
        zero2[...] = jnp.zeros_like(zero2)
        fill = [pltpu.make_async_copy(zero13, osp13.at[l], sem.at[6 + l]) for l in range(4)]
        fill += [pltpu.make_async_copy(zero2, osp2.at[l], sem.at[10 + l]) for l in range(4)]
        for copy in fill:
            copy.start()
        for copy in fill:
            copy.wait()

    for copy in copies:
        copy.wait()


def solution(mesh):
    flat_axes = ('stage', 'expert')

    def local_move(w_gate, w_up, w_down, dense, hot_ids, spare_map):
        sources = (w_gate.reshape(4, 4, 64, 512), w_up.reshape(4, 4, 64, 512), w_down.reshape(4, 4, 4, 8, 1024),
                   dense.reshape(2, 512, 1024))
        hbm = pl.BlockSpec(memory_space=pltpu.HBM)
        vmem = pl.BlockSpec(memory_space=pltpu.VMEM)
        smem = pl.BlockSpec(memory_space=pltpu.SMEM)
        unit = (4, 4, 96, 256)
        moved = pl.pallas_call(
            _exchange,
            name='exchange',
            out_shape=(pltpu.VMEM((8,) + unit, BF16), pltpu.VMEM((2, 4) + unit, BF16), pltpu.VMEM((4, 2, 512, 1024), BF16)),
            in_specs=[hbm] * 5,
            out_specs=[vmem] * 3,
            scratch_shapes=[
                pltpu.VMEM((4,) + unit, BF16), pltpu.VMEM(unit, BF16), pltpu.VMEM(unit, BF16), pltpu.VMEM(unit, BF16),
                pltpu.VMEM((4, 4, 48, 256), BF16), pltpu.VMEM((4, 4, 48, 256), BF16),
                pltpu.VMEM((4, 48, 256), BF16), pltpu.VMEM((4, 48, 256), BF16),
                pltpu.VMEM((4, 48, 256), BF16), pltpu.VMEM((4, 48, 256), BF16),
                pltpu.SMEM((2,), jnp.int32),
                pltpu.SemaphoreType.DMA((6,)),
                pltpu.SemaphoreType.DMA((4 * UNIT_CHUNKS + 3 * NEAR_CHUNKS + 28,)),
                pltpu.SemaphoreType.DMA((4,)),
            ],
            compiler_params=pltpu.CompilerParams(collective_id=0, has_side_effects=True, vmem_limit_bytes=16 * 2**20),
        )(*[pltpu.with_memory_space_constraint(part, pltpu.HBM) for part in (*sources, hot_ids)])
        moved = [pltpu.with_memory_space_constraint(part, pltpu.VMEM) for part in moved]
        o13, o2, odn, osp13, osp2 = pl.pallas_call(
            _write,
            name='write',
            out_shape=(
                jax.ShapeDtypeStruct((4, 4, 4, 64, 256), BF16),
                jax.ShapeDtypeStruct((4, 4, 4, 8, 1024), BF16),
                jax.ShapeDtypeStruct((4, 2, 512, 1024), BF16),
                jax.ShapeDtypeStruct((4, 4, 4, 64, 256), BF16),
                jax.ShapeDtypeStruct((4, 4, 4, 8, 1024), BF16),
            ),
            in_specs=[smem] + [vmem] * 3,
            out_specs=[hbm] * 5,
            scratch_shapes=[pltpu.VMEM((4, 4, 64, 256), BF16), pltpu.VMEM((4, 4, 8, 1024), BF16), pltpu.SemaphoreType.DMA((14,))],
            compiler_params=pltpu.CompilerParams(vmem_limit_bytes=4 * 2**20),
        )(spare_map, *moved)
        return (o13.reshape(4, 1, 1024, 256), o2.reshape(4, 1, 128, 1024), odn.reshape(4, 1024, 1024),
                osp13.reshape(4, 1, 1024, 256), osp2.reshape(4, 1, 128, 1024))

    expert_spec = P('stage', 'expert', None, None)
    unit_spec = P(None, flat_axes, None, None)
    return jax.shard_map(
        local_move,
        mesh=mesh,
        in_specs=(expert_spec, expert_spec, expert_spec, P('stage', None, None), P(None), P(flat_axes)),
        out_specs=(unit_spec, unit_spec, P(None, None, None), unit_spec, unit_spec),
        check_vma=False,
    )
```

```python
import jax
import jax.numpy as jnp
from jax import lax
from jax.experimental import pallas as pl
from jax.experimental.pallas import tpu as pltpu
from jax.sharding import PartitionSpec as P

MESH = pl.DeviceIdType.MESH
BF16 = jnp.bfloat16
RING = 4
UNIT_CHUNKS = 8
NEAR_CHUNKS = 8
NEAR_ROWS = 48
SIDE_ROWS = 16


def _exchange(gate, up, down, dense, hot_hbm, b, h, dn, u, give, take_in, cand, rza, ryb, sa, sb, rya, rzb, ids, send, recv, local):
    x = lax.axis_index('stage')
    e = lax.axis_index('expert')
    z, y, c = e // 8, (e % 8) // 2, e % 2

    def ring(v):
        return lax.rem(v + RING, RING)

    def dev(xx, yy, zz, cc):
        return (ring(xx), ring(zz) * 8 + ring(yy) * 2 + cc)

    partner = dev(x, y, z, 1 - c)
    S_YZ, S_X, S_DENSE, S_HOT, S_MID, S_LOW = range(6)
    R_YZ = 0
    R_NEAR = R_YZ + RING * UNIT_CHUNKS
    R_FAR = R_NEAR + 2 * NEAR_CHUNKS
    R_AG2 = R_FAR + NEAR_CHUNKS
    R_AG3 = R_AG2 + 8
    R_SIDE = R_AG3 + 4
    R_CROSS = R_SIDE + 4
    R_X, R_OVER, R_TURN, R_DPASS, R_HPASS, R_SWAP, R_RS1, R_RS2, R_AGX, R_AGF = range(R_CROSS + 2, R_CROSS + 12)
    R_AG1 = R_CROSS + 12

    def remote(src, dst, device, s, r):
        return pltpu.make_async_remote_copy(src_ref=src, dst_ref=dst, send_sem=send.at[s], recv_sem=recv.at[r],
                                            device_id=device, device_id_type=MESH)

    def same(ref, device, s, r):
        return remote(ref, ref, device, s, r)

    def settle(sem, like):
        pltpu.make_async_copy(like, like, sem).wait()

    stays = (z == y) & (c == y // 2)
    own_piece = 2 * (y % 2) + c

    def land(zs):
        return jnp.where(zs == x, x, RING + zs)

    loads = []
    for p in range(4):
        cols = pl.ds(p * 128, 128)
        loads.append(pltpu.make_async_copy(gate.at[:, :, :, cols], u.at[p, :, :, 0:64, 0:128], local.at[0]))
        loads.append(pltpu.make_async_copy(up.at[:, :, :, cols], u.at[p, :, :, 0:64, 128:256], local.at[0]))
        for a in range(4):
            loads.append(pltpu.make_async_copy(down.at[p, :, :, :, pl.ds(256 * a, 256)],
                                               u.at[p, :, :, pl.ds(64 + 8 * a, 8), :], local.at[0]))
    own_cols = pl.ds(pl.multiple_of(own_piece * 128, 128), 128)
    keep = [
        pltpu.make_async_copy(gate.at[:, :, :, own_cols], b.at[land(z), :, :, 0:64, 0:128], local.at[1]),
        pltpu.make_async_copy(up.at[:, :, :, own_cols], b.at[land(z), :, :, 0:64, 128:256], local.at[1]),
    ] + [
        pltpu.make_async_copy(down.at[own_piece, :, :, :, pl.ds(256 * a, 256)],
                              b.at[land(z), :, :, pl.ds(64 + 8 * a, 8), :], local.at[1]) for a in range(4)
    ]
    load_dense = pltpu.make_async_copy(dense, dn.at[x], local.at[2])
    load_ids = pltpu.make_async_copy(hot_hbm, ids, local.at[3])
    load_ids.start()
    for copy in loads:
        copy.start()
    load_dense.start()

    @pl.when(stays)
    def _():
        for copy in keep:
            copy.start()

    bar = pltpu.get_barrier_semaphore()

    def greet(device):
        pl.semaphore_signal(bar, inc=1, device_id=device, device_id_type=MESH)

    for zs in range(RING):
        @pl.when(jnp.logical_not(stays & (z == zs)))
        def _():
            greet(dev(x, z, zs, y // 2))
    for d in (1, 2, 3):
        greet(dev(x + d, y, z, c))
        greet(dev(x, y + d, z, c))
        greet(dev(x, y, z + d, c))
    greet(partner)

    settle(local.at[0], u)
    load_ids.wait()
    hot_c = ids[c]
    give[...] = u[ids[1 - c] % 4]
    pl.semaphore_wait(bar, jnp.where(stays, 13, 14))

    def part(ref, index, q):
        return ref.at[index, q // 2, pl.ds(2 * (q % 2), 2)]

    def yz_self(p):
        return stays & (own_piece == p)

    def yz_go(*chunks):
        for q in chunks:
            for p in range(4):
                @pl.when(jnp.logical_not(yz_self(p)))
                def _():
                    remote(part(u, p, q), part(b, land(z), q), dev(x, 2 * c + p // 2, y, p % 2),
                           S_YZ, R_YZ + z * UNIT_CHUNKS + q).start()

    def yz_arrive(zs, q):
        @pl.when(jnp.logical_not(stays & (zs == z)))
        def _():
            settle(recv.at[R_YZ + zs * UNIT_CHUNKS + q], part(b, land(zs), q))

        if q == 0:
            @pl.when(stays & (zs == z))
            def _():
                settle(local.at[1], b.at[0])

    def x_go(*chunks):
        for q in chunks:
            for d in (1, 3, 2):
                to = ring(x + d)
                yz_arrive(to, q)
                remote(part(b, RING + to, q), part(b, x, q), dev(x + d, y, z, c), S_X, R_X).start()

    def near(layer, j):
        return dn.at[ring(layer), c, pl.ds(NEAR_ROWS * j, NEAR_ROWS)]

    def side(layer, axis, at, lanes=pl.ds(0, 1024)):
        start = NEAR_ROWS * NEAR_CHUNKS + SIDE_ROWS * (RING * axis + ring(at))
        return dn.at[ring(layer), c, pl.ds(pl.multiple_of(start, 8), SIDE_ROWS), lanes]

    def beside(axis, d):
        return dev(x, y, z + d, c) if axis else dev(x, y + d, z, c)

    half = NEAR_CHUNKS // 2

    def dense_wait():
        load_dense.wait()

    def dense_cross():
        for d in (1, -1):
            for axis, at in ((0, y), (1, z)):
                same(side(x, axis, at), dev(x + d, y, z, c), S_DENSE, R_CROSS + (d + 1) // 2).start()

    def dense_over():
        for d in (1, -1):
            settle(recv.at[R_CROSS + (d + 1) // 2], dn.at[0, 0, 0:2 * SIDE_ROWS])
            for axis, at in ((0, y), (1, z)):
                same(side(x - d, axis, at, pl.ds(256 * (1 - d), 512)), dev(x + d, y, z, c), S_DENSE, R_OVER).start()

    def dense_own(*chunks):
        for i in chunks:
            j = (i + half) % NEAR_CHUNKS
            same(near(x, i), dev(x + 1, y, z, c), S_DENSE, R_NEAR + i).start()
            same(near(x, j), dev(x - 1, y, z, c), S_DENSE, R_NEAR + NEAR_CHUNKS + j).start()

    def dense_side():
        settle(recv.at[R_OVER], dn.at[0, 0, 0:2 * SIDE_ROWS])
        for axis, at in ((0, y), (1, z)):
            for d in (1, -1):
                for l in (1, 3, 2):
                    same(side(x + l, axis, at), beside(axis, d), S_DENSE, R_SIDE + 2 * axis + (d + 1) // 2).start()

    def dense_turn():
        for axis, at in ((0, y), (1, z)):
            for d in (1, -1):
                settle(recv.at[R_SIDE + 2 * axis + (d + 1) // 2], b.at[0, 0, 0:2])
                lanes = pl.ds(256 * (1 - d), 512)
                for l in (1, 3, 2):
                    same(side(x + l, axis, at - d, lanes), beside(axis, d), S_DENSE, R_TURN).start()

    def dense_side_end():
        settle(recv.at[R_TURN], b.at[0, 0])
        for l in (1, 3, 2):
            same(dn.at[ring(x + l), c, pl.ds(NEAR_ROWS * NEAR_CHUNKS, 2 * RING * SIDE_ROWS)], partner, S_DENSE, R_DPASS).start()

    def dense_near(*chunks):
        for i in chunks:
            j = (i + half) % NEAR_CHUNKS
            settle(recv.at[R_NEAR + i], near(x - 1, i))
            if i < half:
                same(near(x - 1, i), dev(x + 1, y, z, c), S_DENSE, R_FAR + i).start()
            same(near(x - 1, i), partner, S_DENSE, R_DPASS).start()
            settle(recv.at[R_NEAR + NEAR_CHUNKS + j], near(x + 1, j))
            if j >= half:
                same(near(x + 1, j), dev(x - 1, y, z, c), S_DENSE, R_FAR + j).start()
            same(near(x + 1, j), partner, S_DENSE, R_DPASS).start()

    def dense_far(*chunks):
        for j in chunks:
            settle(recv.at[R_FAR + j], near(x + 2, j))
            same(near(x + 2, j), partner, S_DENSE, R_DPASS).start()

    y_hot, z_hot = (hot_c // 8) % 4, hot_c // 32

    def hot_swap():
        remote(give, take_in, partner, S_HOT, R_SWAP).start()

    def hot_rs1():
        settle(recv.at[R_SWAP], take_in)
        cand[...] = jnp.where((hot_c // 4) % 2 == c, u[hot_c % 4], take_in[...])
        rza[z] = cand[:, z, 0:48]
        ryb[y] = cand[y, :, 48:96]
        for d in (1, 3, 2):
            remote(cand.at[:, ring(z + d), 0:48], rza.at[z], dev(x, y, z + d, c), S_MID, R_RS1).start()
            remote(cand.at[ring(y + d), :, 48:96], ryb.at[y], dev(x, y + d, z, c), S_MID, R_RS1).start()

    def hot_rs2():
        settle(recv.at[R_RS1], b.at[0, 0:3])
        sa[...] = rza[z_hot]
        sb[...] = ryb[y_hot]
        rya[y] = sa[y]
        rzb[z] = sb[z]
        for d in (1, 3, 2):
            remote(sa.at[ring(y + d)], rya.at[y], dev(x, y + d, z, c), S_LOW, R_RS2).start()
            remote(sb.at[ring(z + d)], rzb.at[z], dev(x, y, z + d, c), S_LOW, R_RS2).start()

    def hot_agx():
        settle(recv.at[R_RS2], b.at[0, 0, 0:3])
        h[c, x, y, z, 0:48] = rya[y_hot]
        h[c, x, y, z, 48:96] = rzb[z_hot]
        for d in (1, 3, 2):
            same(h.at[c, x, y, z], dev(x + d, y, z, c), S_LOW, R_AGX).start()

    def hot_ag1():
        settle(recv.at[R_AGX], b.at[0, 0, 0:3])
        for d in (1, -1):
            same(h.at[c, 0:2, y, z], dev(x, y, z + d, c), S_MID, R_AG1 + (d + 1) // 2).start()
            same(h.at[c, 2:4, y, z], dev(x, y + d, z, c), S_MID, R_AG1 + 2 + (d + 1) // 2).start()

    def hot_again():
        for d in (1, -1):
            rows = pl.ds(24 * (1 - d), 48)
            settle(recv.at[R_AG1 + (d + 1) // 2], b.at[0, 0, 0:2])
            same(h.at[c, 0:2, y, ring(z - d), rows], dev(x, y, z + d, c), S_MID, R_AGF).start()
            settle(recv.at[R_AG1 + 2 + (d + 1) // 2], b.at[0, 0, 0:2])
            same(h.at[c, 2:4, ring(y - d), z, rows], dev(x, y + d, z, c), S_MID, R_AGF).start()

    def block(layer, d):
        if layer < 2:
            return h.at[c, layer, ring(y + d)]
        return h.at[c, layer, :, ring(z + d)]

    def along(layer, d):
        return dev(x, y + d, z, c) if layer < 2 else dev(x, y, z + d, c)

    def hot_ag2():
        settle(recv.at[R_AGF], b.at[0, 0])
        for lift in (0, 1):
            for l in (0, 2):
                same(block(l + lift, 0), along(l, 1), S_HOT, R_AG2 + l + lift).start()
                same(block(l + 1 - lift, 0), along(l, -1), S_HOT, R_AG2 + 4 + l + 1 - lift).start()
        for l in range(4):
            same(block(l, 0), partner, S_HOT, R_HPASS).start()

    def hot_ag3(*lifts):
        for lift in lifts:
            for l in (0, 2):
                settle(recv.at[R_AG2 + l + lift], block(l + lift, -1))
                if lift == 0:
                    same(block(l, -1), along(l, 1), S_HOT, R_AG3 + l).start()
                same(block(l + lift, -1), partner, S_HOT, R_HPASS).start()
                settle(recv.at[R_AG2 + 4 + l + 1 - lift], block(l + 1 - lift, 1))
                if lift == 0:
                    same(block(l + 1, 1), along(l, -1), S_HOT, R_AG3 + l + 1).start()
                same(block(l + 1 - lift, 1), partner, S_HOT, R_HPASS).start()

    def hot_end():
        for l in range(4):
            settle(recv.at[R_AG3 + l], block(l, 2))
            same(block(l, 2), partner, S_HOT, R_HPASS).start()

    dense_wait()
    hot_swap()
    yz_go(0)
    dense_cross()
    dense_own(0, 1, 2, 3, 4, 5, 6, 7)
    hot_rs1()
    yz_go(1)
    hot_rs2()
    dense_over()
    yz_go(2)
    dense_near(0)
    hot_agx()
    yz_go(3)
    dense_near(1, 2, 3, 4, 5, 6, 7)
    dense_side()
    x_go(0, 1)
    hot_ag1()
    yz_go(4, 5)
    x_go(2, 3)
    hot_again()
    dense_turn()
    yz_go(6, 7)
    x_go(4, 5)
    hot_ag2()
    x_go(6)
    dense_far(0, 1, 2, 3, 4, 5, 6, 7)
    x_go(7)
    dense_side_end()
    hot_ag3(0, 1)
    hot_end()
    for q in range(UNIT_CHUNKS):
        yz_arrive(x, q)
    settle(recv.at[R_X], b.at[0:3])
    settle(recv.at[R_DPASS], b.at[0:4])
    settle(recv.at[R_HPASS], b.at[0:4])

    @pl.when(stays)
    def _():
        settle(send.at[S_YZ], b.at[0:3])

    @pl.when(jnp.logical_not(stays))
    def _():
        settle(send.at[S_YZ], b.at[0:4])

    settle(send.at[S_X], b.at[0:3])
    settle(send.at[S_DENSE], b)
    settle(send.at[S_HOT], b)
    settle(send.at[S_MID], b.at[0:2, 0:3])
    settle(send.at[S_LOW], b.at[0:2, 0, 0:3])


def _write(spare, b, h, dn, o13, o2, odn, osp13, osp2, zero13, zero2, sem):
    copies = [pltpu.make_async_copy(dn, odn, sem.at[0])]
    copies.append(pltpu.make_async_copy(b.at[0:4, :, :, 0:64], o13, sem.at[1]))
    for a in range(4):
        copies.append(pltpu.make_async_copy(b.at[0:4, :, :, pl.ds(64 + 8 * a, 8)], o2.at[:, :, :, :, pl.ds(256 * a, 256)], sem.at[2 + a]))
    for copy in copies:
        copy.start()
    slot = spare[0]

    @pl.when(slot >= 0)
    def _():
        fill = [pltpu.make_async_copy(h.at[slot, :, :, :, 0:64], osp13, sem.at[6])]
        for a in range(4):
            fill.append(pltpu.make_async_copy(h.at[slot, :, :, :, pl.ds(64 + 8 * a, 8)], osp2.at[:, :, :, :, pl.ds(256 * a, 256)], sem.at[7 + a]))
        for copy in fill:
            copy.start()
        for copy in fill:
            copy.wait()

    @pl.when(slot < 0)
    def _():
        zero13[...] = jnp.zeros_like(zero13)
        zero2[...] = jnp.zeros_like(zero2)
        fill = [pltpu.make_async_copy(zero13, osp13.at[l], sem.at[6 + l]) for l in range(4)]
        fill += [pltpu.make_async_copy(zero2, osp2.at[l], sem.at[10 + l]) for l in range(4)]
        for copy in fill:
            copy.start()
        for copy in fill:
            copy.wait()

    for copy in copies:
        copy.wait()


def solution(mesh):
    flat_axes = ('stage', 'expert')

    def local_move(w_gate, w_up, w_down, dense, hot_ids, spare_map):
        sources = (w_gate.reshape(4, 4, 64, 512), w_up.reshape(4, 4, 64, 512), w_down.reshape(4, 4, 4, 8, 1024),
                   dense.reshape(2, 512, 1024))
        hbm = pl.BlockSpec(memory_space=pltpu.HBM)
        vmem = pl.BlockSpec(memory_space=pltpu.VMEM)
        smem = pl.BlockSpec(memory_space=pltpu.SMEM)
        unit = (4, 4, 96, 256)
        moved = pl.pallas_call(
            _exchange,
            name='exchange',
            out_shape=(pltpu.VMEM((8,) + unit, BF16), pltpu.VMEM((2, 4) + unit, BF16), pltpu.VMEM((4, 2, 512, 1024), BF16)),
            in_specs=[hbm] * 5,
            out_specs=[vmem] * 3,
            scratch_shapes=[
                pltpu.VMEM((4,) + unit, BF16), pltpu.VMEM(unit, BF16), pltpu.VMEM(unit, BF16), pltpu.VMEM(unit, BF16),
                pltpu.VMEM((4, 4, 48, 256), BF16), pltpu.VMEM((4, 4, 48, 256), BF16),
                pltpu.VMEM((4, 48, 256), BF16), pltpu.VMEM((4, 48, 256), BF16),
                pltpu.VMEM((4, 48, 256), BF16), pltpu.VMEM((4, 48, 256), BF16),
                pltpu.SMEM((2,), jnp.int32),
                pltpu.SemaphoreType.DMA((6,)),
                pltpu.SemaphoreType.DMA((4 * UNIT_CHUNKS + 3 * NEAR_CHUNKS + 32,)),
                pltpu.SemaphoreType.DMA((4,)),
            ],
            compiler_params=pltpu.CompilerParams(collective_id=0, has_side_effects=True, vmem_limit_bytes=16 * 2**20),
        )(*[pltpu.with_memory_space_constraint(part, pltpu.HBM) for part in (*sources, hot_ids)])
        moved = [pltpu.with_memory_space_constraint(part, pltpu.VMEM) for part in moved]
        o13, o2, odn, osp13, osp2 = pl.pallas_call(
            _write,
            name='write',
            out_shape=(
                jax.ShapeDtypeStruct((4, 4, 4, 64, 256), BF16),
                jax.ShapeDtypeStruct((4, 4, 4, 8, 1024), BF16),
                jax.ShapeDtypeStruct((4, 2, 512, 1024), BF16),
                jax.ShapeDtypeStruct((4, 4, 4, 64, 256), BF16),
                jax.ShapeDtypeStruct((4, 4, 4, 8, 1024), BF16),
            ),
            in_specs=[smem] + [vmem] * 3,
            out_specs=[hbm] * 5,
            scratch_shapes=[pltpu.VMEM((4, 4, 64, 256), BF16), pltpu.VMEM((4, 4, 8, 1024), BF16), pltpu.SemaphoreType.DMA((14,))],
            compiler_params=pltpu.CompilerParams(vmem_limit_bytes=4 * 2**20),
        )(spare_map, *moved)
        return (o13.reshape(4, 1, 1024, 256), o2.reshape(4, 1, 128, 1024), odn.reshape(4, 1024, 1024),
                osp13.reshape(4, 1, 1024, 256), osp2.reshape(4, 1, 128, 1024))

    expert_spec = P('stage', 'expert', None, None)
    unit_spec = P(None, flat_axes, None, None)
    return jax.shard_map(
        local_move,
        mesh=mesh,
        in_specs=(expert_spec, expert_spec, expert_spec, P('stage', None, None), P(None), P(flat_axes)),
        out_specs=(unit_spec, unit_spec, P(None, None, None), unit_spec, unit_spec),
        check_vma=False,
    )
```
